32 devices in a mesh: dp: 2 (over x), tp: 16 (over y, z, core).
Axes of the slice: x: 2, y: 2, z: 4, core: 2. Of those that a mesh axis runs over, the one named last changes fastest.
Arguments:
- x: bfloat16 [4096, 8192], P('dp'), parts along dimension 0
- w_gate: bfloat16 [8192, 49152], P(None, 'tp')
- w_up: bfloat16 [8192, 49152], P(None, 'tp')
- w_down: bfloat16 [49152, 8192], P('tp')
Outputs:
- output: bfloat16 [4096, 8192], P('dp'), parts along dimension 0
There are 2 independent parts. The reference program is written for one: setup_inputs(seed, part) draws one part's arguments, and reference() takes and returns one part's arrays. A program takes and returns all parts, laid end to end along the dimension named above; an argument that names none is the same for every part.
All inputs are finite; a program needn't handle non-finite values.
Results may differ from the reference program's by a relative error of at most 0.016.
Values are sent between devices in bfloat16 or wider.
A program may use at most 2 GiB of HBM per device.

```python
import jax
import jax.numpy as jnp

ROWS = 2048
D = 8192
FF = 49152


def setup_inputs(seed: int = 0, part: int = 0) -> dict:
    kx, kg, ku, kd = jax.random.split(jax.random.key(seed), 4)
    drawn = {
        "x": jax.random.normal(jax.random.fold_in(kx, part), (ROWS, D), jnp.float32),
        "w_gate": jax.random.normal(kg, (D, FF), jnp.float32) * D**-0.5,
        "w_up": jax.random.normal(ku, (D, FF), jnp.float32) * D**-0.5,
        "w_down": jax.random.normal(kd, (FF, D), jnp.float32) * FF**-0.5,
    }
    return {k: v.astype(jnp.bfloat16) for k, v in drawn.items()}


def reference(x, w_gate, w_up, w_down):
    gate = jnp.dot(x, w_gate, preferred_element_type=jnp.float32)
    up = jnp.dot(x, w_up, preferred_element_type=jnp.float32)
    hidden = (jax.nn.silu(gate) * up).astype(jnp.bfloat16)
    return jnp.dot(hidden, w_down, preferred_element_type=jnp.float32).astype(jnp.bfloat16)
```

```python
import jax
import jax.numpy as jnp
from jax import lax
from jax.experimental import pallas as pl
from jax.sharding import PartitionSpec as P

PARTS = ((1, ((1, "call"),)),) * 3 + ((1, ((1, "swap"), (1, "call"))),)
Y, ZFAR, ZNEAR, CORE = 0, 1, 2, 3
BIT = {Y: 8, ZFAR: 4, ZNEAR: 2, CORE: 1}
COLOURS = ((Y, ZNEAR, ZFAR), (ZNEAR, Y, ZFAR))
STEPS = (1, 1, 2)
CALL_STEPS = 5


def room(shape):
    return pl.pallas_call(
        lambda out: None,
        out_shape=jax.ShapeDtypeStruct(shape, jnp.bfloat16),
        out_specs=pl.BlockSpec(memory_space=pl.ANY),
        name="room",
    )()


def solution(mesh):
    size = mesh.shape["tp"]

    def swap(a, axis):
        return lax.ppermute(a, "tp", [(i, i ^ BIT[axis]) for i in range(size)])

    def step(x, w_gate, w_up, w_down):
        me = lax.axis_index("tp")
        bits = {axis: (me // BIT[axis]) % 2 for axis in BIT}
        rows_all, d = x.shape[0], w_down.shape[1]
        box = {"y": room((rows_all, d)), "jobs": [], "acc": {}}

        def pick(a, axis, which):
            return lax.dynamic_slice_in_dim(a, which, 1, axis=axis)

        def total(addends, chosen, n, half):
            def part(a):
                starts = [chosen.get(k, 0) if a.shape[k] > 1 else 0 for k in (0, 1, 2)]
                sizes = [1 if k in chosen else a.shape[k] for k in (0, 1, 2)]
                first = n * half if a.shape[4] > half else 0
                cut = lax.dynamic_slice(
                    a, (*starts, 0, first), (*sizes, a.shape[3], half)
                )
                return cut.astype(jnp.float32)

            return sum(part(a) for a in addends[1:]) + part(addends[0])

        def job(key, sent, row, col, rows, width, how):
            got = (yield [(sent, CORE)], 1)[0]
            small, half = rows // 16, width // 2
            view = (2, 2, 2, small, width)
            both = [box["acc"].pop(key).reshape(view), got.reshape(view)]
            addends = [list(both), list(both)]
            chosen = [{}, {}]
            for stage, steps in enumerate(STEPS):
                moved = []
                for n, order in enumerate(COLOURS):
                    axis = order[stage]
                    theirs = {**chosen[n], axis: 1 - bits[axis]}
                    out = total(addends[n], theirs, n, half).astype(jnp.bfloat16)
                    chosen[n][axis] = bits[axis]
                    moved.append((out, axis))
                back = yield moved, steps
                for n in (0, 1):
                    addends[n].append(back[n])
            accs = [total(addends[n], chosen[n], n, half) for n in (0, 1)]
            parts = [a.astype(jnp.bfloat16).reshape(small, half) for a in accs]
            if how == "call":
                whole = jnp.concatenate(parts, 1)
                done = (yield [(whole, None)], CALL_STEPS)[0]
                box["y"] = lax.dynamic_update_slice(box["y"], done, (row, col))
                return
            parts = [p.reshape(1, 1, 1, 1, small, half) for p in parts]
            for stage in (3, 2, 1, 0):
                axes = [(CORE, *order)[stage] for order in COLOURS]
                back = yield list(zip(parts, axes)), 1
                for n, axis in enumerate(axes):
                    first = bits[axis] == 0
                    ours, theirs = parts[n], back[n]
                    parts[n] = jnp.concatenate(
                        [jnp.where(first, ours, theirs), jnp.where(first, theirs, ours)],
                        axis,
                    )
            for n, p in enumerate(parts):
                box["y"] = lax.dynamic_update_slice(
                    box["y"], p.reshape(rows, half), (row, col + n * half)
                )

        def send(a, axis):
            if axis is None:
                return lax.all_gather(a, "tp", axis=0, tiled=True)
            return swap(a, axis)

        def begin(*args):
            it = job(*args)
            moved, steps = next(it)
            box["jobs"].append([it, moved, steps, None])

        def launch():
            for entry in box["jobs"]:
                if entry[3] is None:
                    entry[3] = [send(*m) for m in entry[1]]

        def advance(entry, got):
            try:
                entry[1], entry[2] = entry[0].send(got)
                entry[3] = None
            except StopIteration:
                box["jobs"].remove(entry)

        def compute(f, a, *rest, key=None):
            new = [e for e in box["jobs"] if e[3] is None]
            a, ready = lax.optimization_barrier((a, [[m[0] for m in e[1]] for e in new]))
            for entry, arrays in zip(new, ready):
                entry[1] = [(r, m[1]) for r, m in zip(arrays, entry[1])]
            launch()
            result = f(a, *rest)
            due = []
            for entry in box["jobs"]:
                entry[2] -= 1
                if entry[2] == 0:
                    due.append(entry)
            result, arrays = lax.optimization_barrier((result, [e[3] for e in due]))
            if key is not None:
                box["acc"][key] = result
            for entry, got in zip(due, arrays):
                advance(entry, got)
            return result

        def matmul(a, w):
            return jnp.dot(a, w, preferred_element_type=jnp.float32)

        row = 0
        key = 0
        for share, cuts in PARTS:
            rows = rows_all * share // sum(s for s, _ in PARTS)
            own = slice(row, row + rows)
            gate = compute(lambda a, w: matmul(a[own], w), x, w_gate)
            x, gate = lax.optimization_barrier((x, gate))
            hidden = compute(
                lambda a, g, w: (jax.nn.silu(g) * matmul(a[own], w)).astype(jnp.bfloat16),
                x,
                gate,
                w_up,
            )
            view = hidden.reshape(8, 2, rows // 16, hidden.shape[1])
            away = pick(view, 1, 1 - bits[CORE]).reshape(rows // 2, -1)
            home = pick(view, 1, bits[CORE]).reshape(rows // 2, -1)
            col = 0
            for part, how in cuts:
                width = d * part // sum(p for p, _ in cuts)
                w = w_down[:, col : col + width]
                sent = compute(lambda a, w: matmul(a, w).astype(jnp.bfloat16), away, w)
                begin(key, sent, row, col, rows, width, how)
                compute(matmul, home, w, key=key)
                col += width
                key += 1
            row += rows
        while box["jobs"]:
            new = [e for e in box["jobs"] if e[3] is None]
            ready = lax.optimization_barrier([[m[0] for m in e[1]] for e in new])
            for entry, arrays in zip(new, ready):
                entry[1] = [(r, m[1]) for r, m in zip(arrays, entry[1])]
            launch()
            called = [e for e in box["jobs"] if e[1][0][1] is None]
            due = [e for e in box["jobs"] if e[1][0][1] is not None]
            for entry in called:
                entry[2] -= 1
                if entry[2] <= 0 or len(called) == len(box["jobs"]):
                    due.append(entry)
            arrays = lax.optimization_barrier([e[3] for e in due])
            for entry, got in zip(due, arrays):
                advance(entry, got)
        return box["y"]

    return jax.shard_map(
        step,
        mesh=mesh,
        in_specs=(P("dp", None), P(None, "tp"), P(None, "tp"), P("tp", None)),
        out_specs=P("dp", None),
        check_vma=False,
    )
```
